256 devices in a mesh: grp: 2 (over y), row: 64 (over x, z), col: 2 (over core).
Axes of the slice: x: 4, y: 2, z: 16, core: 2. Of those that a mesh axis runs over, the one named last changes fastest.
The devices are a block of a 4x16x16 slice.
Arguments:
- queries: bfloat16 [65536, 2, 128], P(('grp', 'row', 'col')), parts along dimension 0, may hold values from -6 to 6
- keys: bfloat16 [65536, 2, 128], P(('grp', 'row', 'col')), parts along dimension 0, may hold values from -6 to 6
- values: bfloat16 [65536, 2, 128], P(('grp', 'row', 'col')), parts along dimension 0, may hold values from -6 to 6
Outputs:
- attended: bfloat16 [65536, 256], P(('grp', 'row', 'col')), parts along dimension 0
The draws below stay inside these ranges and needn't reach their ends.
There are 2 independent parts, one for each index of `grp`. The reference program is written for one: setup_inputs(seed, part) draws one part's arguments, and reference() takes and returns one part's arrays. A program takes and returns all parts, laid end to end along the dimension named above; each array names one. Nothing has to cross between parts.
All inputs are finite; a program needn't handle non-finite values.
Results may differ from the reference program's by a relative error of at most 0.014.
Values may be sent and summed in bfloat16 or wider, within the bound.
No kernel may reach another device: no remote copies, remote signals or barrier semaphores. Data moves between devices by JAX's collectives and lax.ppermute only.
A program may use at most 128 MiB of HBM per device.

```python
import jax
import jax.numpy as jnp
from jax import lax

HEAD = 128
HEADS = 2
TOKENS = 32768


def make_pairs(key):
    first, second = jax.random.split(jax.random.fold_in(key, 7), 2)
    shape = (TOKENS, HEADS, HEAD)
    query_draw = jnp.clip(jax.random.normal(first, shape, jnp.float32) * 1.732, -6.0, 6.0)
    key_draw = jnp.clip(jax.random.normal(second, shape, jnp.float32) * 1.732, -6.0, 6.0)
    return (query_draw, key_draw)


def draw_queries(key, part):
    return make_pairs(key)[0].astype(jnp.bfloat16)


def draw_keys(key, part):
    return make_pairs(key)[1].astype(jnp.bfloat16)


def level_of(rng, shape, shards, smallest, high):
    factor_of, own = 1.0, jax.random.fold_in(rng, 6)
    for axis_at, blocks in shards:
        steps = jnp.exp(jax.random.uniform(jax.random.fold_in(own, axis_at), (blocks,), jnp.float32, smallest / len(shards), high / len(shards)))
        factor_of = factor_of * jnp.repeat(steps, shape[axis_at] // blocks).reshape([-1 if axis == axis_at else 1 for axis in range(len(shape))])
    return factor_of


def scatter_about(own_key, dims, deviation, limit, shards=(), kind=jnp.bfloat16):
    level = level_of(own_key, dims, shards, -0.22, 0.18) if shards else 1.0
    values = jax.random.normal(own_key, dims, jnp.float32) * deviation * level
    return jnp.minimum(jnp.maximum(values, -limit), limit).astype(kind)


def setup_inputs(seed: int = 0, part: int = 0) -> dict:
    arg_keys = jax.random.split(jax.random.key(seed), 4)
    part_splits = jax.random.split(jax.random.fold_in(arg_keys[3], part), 4)
    return {
        "queries": draw_queries(jax.random.fold_in(jax.random.fold_in(arg_keys[3], part), 71), part),
        "keys": draw_keys(jax.random.fold_in(jax.random.fold_in(arg_keys[3], part), 71), part),
        "values": scatter_about(part_splits[2], (TOKENS, HEADS, HEAD), 1.0, 6.0, ((0, 128),)),
    }


def reference(queries, keys, values):
    scale = HEAD ** -0.5
    key_full = keys.astype(jnp.float32)
    value_full = values.astype(jnp.float32)
    length = min(512, TOKENS)
    query_blocks = queries.reshape(TOKENS // length, length, HEADS, HEAD)

    def one_block(query_block):
        score = jnp.einsum("qhd,khd->hqk", query_block.astype(jnp.float32), key_full, precision=lax.Precision.HIGHEST) * scale
        peak = jnp.max(score, axis=-1)
        weight = jnp.exp(score - peak[..., None]).astype(jnp.bfloat16)
        total = jnp.sum(weight.astype(jnp.float32), axis=-1)
        mixed = jnp.einsum("hqk,khd->qhd", weight.astype(jnp.float32), value_full, precision=lax.Precision.HIGHEST)
        result = mixed / jnp.transpose(total)[..., None]
        return result.reshape(length, HEADS * HEAD).astype(jnp.bfloat16)

    return lax.map(one_block, query_blocks).reshape(TOKENS, HEADS * HEAD)
```

```python
import functools
import math

import jax
import jax.numpy as jnp
from jax import lax
from jax.experimental import pallas as pl
from jax.experimental.pallas import tpu as pltpu
from jax.sharding import Mesh
from jax.sharding import PartitionSpec as P


ROW_X = 4
BLOCK = 512
STAT_ROWS = 16
VMEM = pl.BlockSpec(memory_space=pltpu.VMEM)
SMEM = pl.BlockSpec(memory_space=pltpu.SMEM)
NT = (((1,), (1,)), ((), ()))


def fold_kernel(*refs, pieces, heads, width, block, first):
    kv_refs, q_ref = refs[:pieces], refs[pieces]
    if first:
        acc_out, stat_out, v_turned, score = refs[pieces + 1 :]
    else:
        acc_in, stat_in, acc_out, stat_out, v_turned, score = refs[pieces + 1 :]
    rows = kv_refs[0].shape[0] // 2
    scale = width ** (-0.5) * math.log2(math.e)
    n_blocks = acc_out.shape[2] // block
    for h in range(heads):
        lanes = slice(h * width, (h + 1) * width)
        for i in range(pieces):
            v_turned[h, :, i * rows : (i + 1) * rows] = kv_refs[i][rows:, lanes].T

    def span(j):
        return pl.ds(pl.multiple_of(j * block, block), block)

    def score_of(h, j):
        lanes = slice(h * width, (h + 1) * width)
        q = q_ref[h, span(j), :]
        for i in range(pieces):
            s = lax.dot_general(kv_refs[i][:rows, lanes], q, NT, preferred_element_type=jnp.float32)
            score[h, i * rows : (i + 1) * rows, :] = s * scale

    def finish(h, j):
        at = span(j)
        s = score[h]
        top = s.max(axis=0, keepdims=True)
        if not first:
            top = jnp.maximum(top, stat_in[h, 0:1, at])
        p = jnp.exp2(s - top)
        total = p.sum(axis=0, keepdims=True)
        mixed = jnp.dot(v_turned[h], p.astype(jnp.bfloat16), preferred_element_type=jnp.float32)
        if not first:
            fade = jnp.exp2(stat_in[h, 0:1, at] - top)
            total = total + stat_in[h, 1:2, at] * fade
            mixed = mixed + acc_in[h, :, at] * fade
        acc_out[h, :, at] = mixed
        stat_out[h, 0:1, at] = top
        stat_out[h, 1:2, at] = total

    score_of(0, 0)

    def step(j, _):
        for h in range(heads):
            if h + 1 < heads:
                score_of(h + 1, j)
            else:
                score_of(0, jnp.minimum(j + 1, n_blocks - 1))
            finish(h, j)
        return 0

    lax.fori_loop(0, n_blocks, step, 0)


def fold(state, chunks, queries, count=None):
    pieces, rows = len(chunks), chunks[0].shape[0] // 2
    heads, everyone, width = queries.shape
    count = everyone if count is None else count
    first = state is None
    operands = [*chunks, queries, *(() if first else state)]
    aliases = {} if first or count < everyone else {pieces + 1: 0, pieces + 2: 1}
    flops = 4 * heads * width * count * rows * pieces
    return pl.pallas_call(
        functools.partial(
            fold_kernel, pieces=pieces, heads=heads, width=width, block=BLOCK, first=first
        ),
        out_shape=(
            jax.ShapeDtypeStruct((heads, width, count), jnp.float32),
            jax.ShapeDtypeStruct((heads, 8, count), jnp.float32),
        ),
        in_specs=[VMEM] * len(operands),
        out_specs=(VMEM, VMEM),
        scratch_shapes=[
            pltpu.VMEM((heads, width, pieces * rows), jnp.bfloat16),
            pltpu.VMEM((heads, pieces * rows, BLOCK), jnp.float32),
        ],
        input_output_aliases=aliases,
        compiler_params=pltpu.CompilerParams(vmem_limit_bytes=8 * 2**20),
        cost_estimate=pl.CostEstimate(
            flops=flops, transcendentals=heads * count * rows * pieces, bytes_accessed=0
        ),
        name="fold",
    )(*operands)


def lay_kernel(*refs, heads, width):
    pieces, out_ref = refs[:-1], refs[-1]
    rows = pieces[0].shape[0]
    for at, part in enumerate(pieces):
        for h in range(heads):
            out_ref[h, at * rows : (at + 1) * rows, :] = part[:, h * width : (h + 1) * width]


def lay(pieces, heads):
    rows, lanes = pieces[0].shape
    width = lanes // heads
    return pl.pallas_call(
        functools.partial(lay_kernel, heads=heads, width=width),
        out_shape=jax.ShapeDtypeStruct((heads, len(pieces) * rows, width), pieces[0].dtype),
        in_specs=[VMEM] * len(pieces),
        out_specs=VMEM,
        compiler_params=pltpu.CompilerParams(vmem_limit_bytes=4 * 2**20),
        name="lay",
    )(*pieces)


def log_weight(stats, h):
    at = 3 * h
    return stats[at : at + 1] + stats[at + 1 : at + 2] + stats[at + 2 : at + 3]


def pack_kernel(dest_ref, acc_ref, stat_ref, *refs, heads, width, own, start):
    (more_ref, out_ref) = refs if len(refs) == 2 else (None, refs[0])
    owners = out_ref.shape[0]
    count = owners * own
    at = slice(start, start + count)
    which = lax.broadcasted_iota(jnp.int32, (STAT_ROWS, count), 0)
    stats = jnp.zeros((STAT_ROWS, count), jnp.float32)
    scales = []
    for h in range(heads):
        top, total = stat_ref[h, 0:1, at], stat_ref[h, 1:2, at]
        fade = share = None
        if more_ref is not None:
            log = jnp.concatenate(
                [log_weight(more_ref[j, heads * width :, :].astype(jnp.float32), h) for j in range(owners)],
                axis=1,
            )
            raised = jnp.maximum(top, log)
            fade, share = jnp.exp2(top - raised), jnp.exp2(log - raised)
            total, top = total * fade + share, raised
        weight = 1.0 / total
        scales.append((weight, None) if fade is None else (fade * weight, share * weight))
        rest = top + jnp.log2(total)
        for part in range(3):
            rounded = rest.astype(jnp.bfloat16).astype(jnp.float32)
            stats = jnp.where(which == 3 * h + part, rounded, stats)
            rest = rest - rounded
    stats = stats.astype(jnp.bfloat16)
    for j in range(owners):
        to, here = dest_ref[j], slice(j * own, (j + 1) * own)
        out_ref[to, heads * width :, :] = stats[:, here]
        for h in range(heads):
            rows = slice(h * width, (h + 1) * width)
            keep, add = scales[h]
            mixed = acc_ref[h, :, start + j * own : start + (j + 1) * own] * keep[:, here]
            if add is not None:
                mixed = mixed + more_ref[j, rows, :].astype(jnp.float32) * add[:, here]
            out_ref[to, rows, :] = mixed.astype(jnp.bfloat16)


def pack(dest, state, heads, own, start=0, more=None):
    acc, stat = state
    width, count = acc.shape[1], acc.shape[2]
    more = () if more is None else (more,)
    return pl.pallas_call(
        functools.partial(pack_kernel, heads=heads, width=width, own=own, start=start),
        out_shape=jax.ShapeDtypeStruct(
            ((count - start) // own, heads * width + STAT_ROWS, own), jnp.bfloat16
        ),
        in_specs=[SMEM, VMEM, VMEM] + [VMEM] * len(more),
        out_specs=VMEM,
        compiler_params=pltpu.CompilerParams(vmem_limit_bytes=4 * 2**20),
        name="pack",
    )(dest, acc, stat, *more)


def merge_kernel(in_ref, out_ref, *, heads, width):
    sources = in_ref.shape[0]
    for h in range(heads):
        logs = [
            log_weight(in_ref[i, heads * width :, :].astype(jnp.float32), h) for i in range(sources)
        ]
        top = functools.reduce(jnp.maximum, logs)
        shares = [jnp.exp2(x - top) for x in logs]
        total = functools.reduce(jnp.add, shares)
        mixed = None
        for i in range(sources):
            part = in_ref[i, h * width : (h + 1) * width, :].astype(jnp.float32) * (shares[i] / total)
            mixed = part if mixed is None else mixed + part
        out_ref[:, h * width : (h + 1) * width] = mixed.T.astype(jnp.bfloat16)


def merge(parts, heads, width):
    return pl.pallas_call(
        functools.partial(merge_kernel, heads=heads, width=width),
        out_shape=jax.ShapeDtypeStruct((parts.shape[2], heads * width), jnp.bfloat16),
        in_specs=[VMEM],
        out_specs=VMEM,
        compiler_params=pltpu.CompilerParams(vmem_limit_bytes=4 * 2**20),
        name="merge",
    )(parts)


def body(queries, keys, values):
    own, heads, width = queries.shape
    n_x, n_z, n_col = (lax.axis_size(a) for a in ("x", "z", "col"))
    swap = functools.partial(lax.ppermute, axis_name="col", perm=[(c, n_col - 1 - c) for c in range(n_col)])
    along = [
        (z * n_col + c, (z + (1 if c == 0 else -1)) % n_z * n_col + c)
        for z in range(n_z)
        for c in range(n_col)
    ]
    forward = functools.partial(lax.ppermute, axis_name=("z", "col"), perm=along)
    here = jnp.concatenate([keys, values], axis=0).reshape(2 * own, heads * width)
    q = lax.optimization_barrier((queries, here))[0].reshape(own, heads * width)
    ahead = forward(here)
    other = swap(here)
    chunk = [ahead, forward(other)]

    q_mine = [q]
    for d in (1, n_x - 1, *range(2, n_x - 1)):
        q_mine.append(lax.ppermute(q, "x", [(x, (x + d) % n_x) for x in range(n_x)]))
    offsets = [0, 1, n_x - 1, *range(2, n_x - 1)]
    q_theirs = [swap(a) for a in q_mine]
    q_all = lay(q_mine + q_theirs, heads)

    state = fold(None, [here, *chunk], q_all)
    last = n_z // 2
    for _ in range(2, last):
        chunk = [forward(a) for a in chunk]
        state = fold(state, chunk, q_all)
    share = q_all.shape[1] // n_col
    sent = swap(pack(jnp.arange(n_x, dtype=jnp.int32), state, heads, own, start=share))
    chunk = forward(chunk[0])
    other = swap(chunk)
    mine = fold(state, [chunk, other], q_all, share)

    x = lax.axis_index("x")
    dest = jnp.stack([x - d for d in offsets]) % n_x
    parts = pack(dest.astype(jnp.int32), mine, heads, own, more=sent)
    parts = lax.all_to_all(parts, "x", 0, 0, tiled=True)
    return merge(parts, heads, width)


def solution(mesh):
    n_grp, n_row, n_col = mesh.devices.shape
    n_z = n_row // ROW_X
    split = Mesh(mesh.devices.reshape(n_grp, ROW_X, n_z, n_col), ("grp", "x", "z", "col"))
    everywhere = ("grp", "x", "z", "col")

    return jax.shard_map(
        body,
        mesh=split,
        in_specs=(P(everywhere, None, None),) * 3,
        out_specs=P(everywhere, None),
        check_vma=False,
    )
```

```python
import functools
import math

import jax
import jax.numpy as jnp
from jax import lax
from jax.experimental import pallas as pl
from jax.experimental.pallas import tpu as pltpu
from jax.sharding import Mesh
from jax.sharding import PartitionSpec as P


ROW_X = 4
BLOCK = 512
STAT_ROWS = 16
VMEM = pl.BlockSpec(memory_space=pltpu.VMEM)
NT = (((1,), (1,)), ((), ()))


def fold_kernel(*refs, pieces, heads, width, block, first):
    kv_refs, q_ref = refs[:pieces], refs[pieces]
    if first:
        acc_out, stat_out, v_turned, score = refs[pieces + 1 :]
    else:
        acc_in, stat_in, acc_out, stat_out, v_turned, score = refs[pieces + 1 :]
    rows = kv_refs[0].shape[0] // 2
    scale = width ** (-0.5) * math.log2(math.e)
    n_blocks = acc_out.shape[2] // block
    for h in range(heads):
        lanes = slice(h * width, (h + 1) * width)
        for i in range(pieces):
            v_turned[h, :, i * rows : (i + 1) * rows] = kv_refs[i][rows:, lanes].T

    def span(j):
        return pl.ds(pl.multiple_of(j * block, block), block)

    def score_of(h, j):
        lanes = slice(h * width, (h + 1) * width)
        q = q_ref[h, span(j), :]
        for i in range(pieces):
            s = lax.dot_general(kv_refs[i][:rows, lanes], q, NT, preferred_element_type=jnp.float32)
            score[h, i * rows : (i + 1) * rows, :] = s * scale

    def finish(h, j):
        at = span(j)
        s = score[h]
        top = s.max(axis=0, keepdims=True)
        if not first:
            top = jnp.maximum(top, stat_in[h, 0:1, at])
        p = jnp.exp2(s - top)
        total = p.sum(axis=0, keepdims=True)
        mixed = jnp.dot(v_turned[h], p.astype(jnp.bfloat16), preferred_element_type=jnp.float32)
        if not first:
            fade = jnp.exp2(stat_in[h, 0:1, at] - top)
            total = total + stat_in[h, 1:2, at] * fade
            mixed = mixed + acc_in[h, :, at] * fade
        acc_out[h, :, at] = mixed
        stat_out[h, 0:1, at] = top
        stat_out[h, 1:2, at] = total

    score_of(0, 0)

    def step(j, _):
        for h in range(heads):
            if h + 1 < heads:
                score_of(h + 1, j)
            else:
                score_of(0, jnp.minimum(j + 1, n_blocks - 1))
            finish(h, j)
        return 0

    lax.fori_loop(0, n_blocks, step, 0)


def fold(state, chunks, queries, count=None):
    pieces, rows = len(chunks), chunks[0].shape[0] // 2
    heads, everyone, width = queries.shape
    count = everyone if count is None else count
    first = state is None
    operands = [*chunks, queries, *(() if first else state)]
    aliases = {} if first or count < state[0].shape[2] else {pieces + 1: 0, pieces + 2: 1}
    flops = 4 * heads * width * count * rows * pieces
    return pl.pallas_call(
        functools.partial(
            fold_kernel, pieces=pieces, heads=heads, width=width, block=BLOCK, first=first
        ),
        out_shape=(
            jax.ShapeDtypeStruct((heads, width, count), jnp.float32),
            jax.ShapeDtypeStruct((heads, 8, count), jnp.float32),
        ),
        in_specs=[VMEM] * len(operands),
        out_specs=(VMEM, VMEM),
        scratch_shapes=[
            pltpu.VMEM((heads, width, pieces * rows), jnp.bfloat16),
            pltpu.VMEM((heads, pieces * rows, BLOCK), jnp.float32),
        ],
        input_output_aliases=aliases,
        compiler_params=pltpu.CompilerParams(vmem_limit_bytes=8 * 2**20),
        cost_estimate=pl.CostEstimate(
            flops=flops, transcendentals=heads * count * rows * pieces, bytes_accessed=0
        ),
        name="fold",
    )(*operands)


def lay_kernel(*refs, heads, width):
    pieces, out_ref = refs[:-1], refs[-1]
    rows = pieces[0].shape[0]
    for at, part in enumerate(pieces):
        for h in range(heads):
            out_ref[h, at * rows : (at + 1) * rows, :] = part[:, h * width : (h + 1) * width]


def lay(pieces, heads):
    rows, lanes = pieces[0].shape
    width = lanes // heads
    return pl.pallas_call(
        functools.partial(lay_kernel, heads=heads, width=width),
        out_shape=jax.ShapeDtypeStruct((heads, len(pieces) * rows, width), pieces[0].dtype),
        in_specs=[VMEM] * len(pieces),
        out_specs=VMEM,
        compiler_params=pltpu.CompilerParams(vmem_limit_bytes=4 * 2**20),
        name="lay",
    )(*pieces)


def log_weight(stats, h):
    at = 3 * h
    return stats[at : at + 1] + stats[at + 1 : at + 2] + stats[at + 2 : at + 3]


def pack_kernel(acc_ref, stat_ref, *refs, heads, width, own, start, owners):
    more_refs, out_refs = refs[:-owners], refs[-owners:]
    count = owners * own
    at = slice(start, start + count)
    which = lax.broadcasted_iota(jnp.int32, (STAT_ROWS, count), 0)
    stats = jnp.zeros((STAT_ROWS, count), jnp.float32)
    scales = []
    for h in range(heads):
        top, total = stat_ref[h, 0:1, at], stat_ref[h, 1:2, at]
        fade = share = None
        if more_refs:
            log = jnp.concatenate(
                [log_weight(more_refs[j][heads * width :, :].astype(jnp.float32), h) for j in range(owners)],
                axis=1,
            )
            raised = jnp.maximum(top, log)
            fade, share = jnp.exp2(top - raised), jnp.exp2(log - raised)
            total, top = total * fade + share, raised
        weight = 1.0 / total
        scales.append((weight, None) if fade is None else (fade * weight, share * weight))
        rest = top + jnp.log2(total)
        for part in range(3):
            rounded = rest.astype(jnp.bfloat16).astype(jnp.float32)
            stats = jnp.where(which == 3 * h + part, rounded, stats)
            rest = rest - rounded
    stats = stats.astype(jnp.bfloat16)
    for j in range(owners):
        out_ref, here = out_refs[j], slice(j * own, (j + 1) * own)
        out_ref[heads * width :, :] = stats[:, here]
        for h in range(heads):
            rows = slice(h * width, (h + 1) * width)
            keep, add = scales[h]
            mixed = acc_ref[h, :, start + j * own : start + (j + 1) * own] * keep[:, here]
            if add is not None:
                mixed = mixed + more_refs[j][rows, :].astype(jnp.float32) * add[:, here]
            out_ref[rows, :] = mixed.astype(jnp.bfloat16)


def pack(state, heads, own, start=0, more=()):
    acc, stat = state
    width, count = acc.shape[1], acc.shape[2]
    owners = (count - start) // own
    message = jax.ShapeDtypeStruct((heads * width + STAT_ROWS, own), jnp.bfloat16)
    return pl.pallas_call(
        functools.partial(pack_kernel, heads=heads, width=width, own=own, start=start, owners=owners),
        out_shape=(message,) * owners,
        in_specs=[VMEM] * (2 + len(more)),
        out_specs=(VMEM,) * owners,
        compiler_params=pltpu.CompilerParams(vmem_limit_bytes=4 * 2**20),
        name="pack",
    )(acc, stat, *more)


def merge_kernel(*refs, heads, width):
    in_refs, out_ref = refs[:-1], refs[-1]
    for h in range(heads):
        logs = [
            log_weight(part[heads * width :, :].astype(jnp.float32), h) for part in in_refs
        ]
        top = functools.reduce(jnp.maximum, logs)
        shares = [jnp.exp2(x - top) for x in logs]
        total = functools.reduce(jnp.add, shares)
        mixed = None
        for ref, share in zip(in_refs, shares):
            part = ref[h * width : (h + 1) * width, :].astype(jnp.float32) * (share / total)
            mixed = part if mixed is None else mixed + part
        out_ref[:, h * width : (h + 1) * width] = mixed.T.astype(jnp.bfloat16)


def merge(parts, heads, width):
    return pl.pallas_call(
        functools.partial(merge_kernel, heads=heads, width=width),
        out_shape=jax.ShapeDtypeStruct((parts[0].shape[1], heads * width), jnp.bfloat16),
        in_specs=[VMEM] * len(parts),
        out_specs=VMEM,
        compiler_params=pltpu.CompilerParams(vmem_limit_bytes=4 * 2**20),
        name="merge",
    )(*parts)


def body(queries, keys, values):
    own, heads, width = queries.shape
    n_x, n_z, n_col = (lax.axis_size(a) for a in ("x", "z", "col"))
    swap = functools.partial(lax.ppermute, axis_name="col", perm=[(c, n_col - 1 - c) for c in range(n_col)])
    along = [
        (z * n_col + c, (z + (1 if c == 0 else -1)) % n_z * n_col + c)
        for z in range(n_z)
        for c in range(n_col)
    ]
    forward = functools.partial(lax.ppermute, axis_name=("z", "col"), perm=along)
    here = jnp.concatenate([keys, values], axis=0).reshape(2 * own, heads * width)
    q = lax.optimization_barrier((queries, here))[0].reshape(own, heads * width)
    ahead = forward(here)
    other = swap(here)
    chunk = [ahead, forward(other)]

    q_mine = [q]
    for d in (1, n_x - 1, *range(2, n_x - 1)):
        q_mine.append(lax.ppermute(q, "x", [(x, (x + d) % n_x) for x in range(n_x)]))
    offsets = [0, 1, n_x - 1, *range(2, n_x - 1)]
    q_theirs = [swap(a) for a in q_mine]
    q_all = lay(q_mine + q_theirs, heads)

    state = fold(None, [here, *chunk], q_all)
    last = n_z // 2
    for _ in range(2, last):
        near = forward(chunk[0])
        chunk = [near, forward(chunk[1])]
        state = fold(state, chunk, q_all)
    share = q_all.shape[1] // n_col
    sent = [swap(a) for a in pack(state, heads, own, start=share)]
    chunk = forward(chunk[0])
    other = swap(chunk)
    mine = fold(state, [chunk], q_all, share)
    mine = fold(mine, [other], q_all, share)

    parts = pack(mine, heads, own, more=sent)
    parts = [parts[0]] + [
        lax.ppermute(a, "x", [(x, (x - d) % n_x) for x in range(n_x)])
        for d, a in zip(offsets[1:], parts[1:])
    ]
    return merge(parts, heads, width)


def solution(mesh):
    n_grp, n_row, n_col = mesh.devices.shape
    n_z = n_row // ROW_X
    split = Mesh(mesh.devices.reshape(n_grp, ROW_X, n_z, n_col), ("grp", "x", "z", "col"))
    everywhere = ("grp", "x", "z", "col")

    return jax.shard_map(
        body,
        mesh=split,
        in_specs=(P(everywhere, None, None),) * 3,
        out_specs=P(everywhere, None),
        check_vma=False,
    )
```

```python
import functools
import math

import jax
import jax.numpy as jnp
from jax import lax
from jax.experimental import pallas as pl
from jax.experimental.pallas import tpu as pltpu
from jax.sharding import Mesh
from jax.sharding import PartitionSpec as P


ROW_X = 4
BLOCK = 512
STAT_ROWS = 16
VMEM = pl.BlockSpec(memory_space=pltpu.VMEM)
NT = (((1,), (1,)), ((), ()))


def fold_kernel(*refs, pieces, heads, width, block, first):
    kv_refs, q_ref = refs[:pieces], refs[pieces]
    if first:
        acc_out, stat_out, v_turned, score = refs[pieces + 1 :]
    else:
        acc_in, stat_in, acc_out, stat_out, v_turned, score = refs[pieces + 1 :]
    rows = kv_refs[0].shape[0] // 2
    scale = width ** (-0.5) * math.log2(math.e)
    n_blocks = acc_out.shape[2] // block
    for h in range(heads):
        lanes = slice(h * width, (h + 1) * width)
        for i in range(pieces):
            v_turned[h, :, i * rows : (i + 1) * rows] = kv_refs[i][rows:, lanes].T

    def span(j):
        return pl.ds(pl.multiple_of(j * block, block), block)

    def score_of(h, j):
        lanes = slice(h * width, (h + 1) * width)
        q = q_ref[h, span(j), :]
        for i in range(pieces):
            s = lax.dot_general(kv_refs[i][:rows, lanes], q, NT, preferred_element_type=jnp.float32)
            score[h, i * rows : (i + 1) * rows, :] = s * scale

    def finish(h, j):
        at = span(j)
        s = score[h]
        top = s.max(axis=0, keepdims=True)
        if not first:
            top = jnp.maximum(top, stat_in[h, 0:1, at])
        p = jnp.exp2(s - top)
        total = p.sum(axis=0, keepdims=True)
        mixed = jnp.dot(v_turned[h], p.astype(jnp.bfloat16), preferred_element_type=jnp.float32)
        if not first:
            fade = jnp.exp2(stat_in[h, 0:1, at] - top)
            total = total + stat_in[h, 1:2, at] * fade
            mixed = mixed + acc_in[h, :, at] * fade
        acc_out[h, :, at] = mixed
        stat_out[h, 0:1, at] = top
        stat_out[h, 1:2, at] = total

    score_of(0, 0)

    def step(j, _):
        for h in range(heads):
            if h + 1 < heads:
                score_of(h + 1, j)
            else:
                score_of(0, jnp.minimum(j + 1, n_blocks - 1))
            finish(h, j)
        return 0

    lax.fori_loop(0, n_blocks, step, 0)


def fold(state, chunks, queries, count=None):
    pieces, rows = len(chunks), chunks[0].shape[0] // 2
    heads, everyone, width = queries.shape
    count = everyone if count is None else count
    first = state is None
    operands = [*chunks, queries, *(() if first else state)]
    aliases = {} if first or count < state[0].shape[2] else {pieces + 1: 0, pieces + 2: 1}
    flops = 4 * heads * width * count * rows * pieces
    return pl.pallas_call(
        functools.partial(
            fold_kernel, pieces=pieces, heads=heads, width=width, block=BLOCK, first=first
        ),
        out_shape=(
            jax.ShapeDtypeStruct((heads, width, count), jnp.float32),
            jax.ShapeDtypeStruct((heads, 8, count), jnp.float32),
        ),
        in_specs=[VMEM] * len(operands),
        out_specs=(VMEM, VMEM),
        scratch_shapes=[
            pltpu.VMEM((heads, width, pieces * rows), jnp.bfloat16),
            pltpu.VMEM((heads, pieces * rows, BLOCK), jnp.float32),
        ],
        input_output_aliases=aliases,
        compiler_params=pltpu.CompilerParams(vmem_limit_bytes=8 * 2**20),
        cost_estimate=pl.CostEstimate(
            flops=flops, transcendentals=heads * count * rows * pieces, bytes_accessed=0
        ),
        name="fold",
    )(*operands)


def lay_kernel(*refs, heads, width):
    pieces, out_ref = refs[:-1], refs[-1]
    rows = pieces[0].shape[0]
    for at, part in enumerate(pieces):
        for h in range(heads):
            out_ref[h, at * rows : (at + 1) * rows, :] = part[:, h * width : (h + 1) * width]


def lay(pieces, heads):
    rows, lanes = pieces[0].shape
    width = lanes // heads
    return pl.pallas_call(
        functools.partial(lay_kernel, heads=heads, width=width),
        out_shape=jax.ShapeDtypeStruct((heads, len(pieces) * rows, width), pieces[0].dtype),
        in_specs=[VMEM] * len(pieces),
        out_specs=VMEM,
        compiler_params=pltpu.CompilerParams(vmem_limit_bytes=4 * 2**20),
        name="lay",
    )(*pieces)


def log_weight(stats, h):
    at = 3 * h
    return stats[at : at + 1] + stats[at + 1 : at + 2] + stats[at + 2 : at + 3]


def pack_kernel(acc_ref, stat_ref, *refs, heads, width, own, start, owners):
    more_refs, out_refs = refs[:-owners], refs[-owners:]
    count = owners * own
    at = slice(start, start + count)
    which = lax.broadcasted_iota(jnp.int32, (STAT_ROWS, count), 0)
    stats = jnp.zeros((STAT_ROWS, count), jnp.float32)
    scales = []
    for h in range(heads):
        top, total = stat_ref[h, 0:1, at], stat_ref[h, 1:2, at]
        fade = share = None
        if more_refs:
            log = jnp.concatenate(
                [log_weight(more_refs[j][heads * width :, :].astype(jnp.float32), h) for j in range(owners)],
                axis=1,
            )
            raised = jnp.maximum(top, log)
            fade, share = jnp.exp2(top - raised), jnp.exp2(log - raised)
            total, top = total * fade + share, raised
        weight = 1.0 / total
        scales.append((weight, None) if fade is None else (fade * weight, share * weight))
        rest = top + jnp.log2(total)
        for part in range(3):
            rounded = rest.astype(jnp.bfloat16).astype(jnp.float32)
            stats = jnp.where(which == 3 * h + part, rounded, stats)
            rest = rest - rounded
    stats = stats.astype(jnp.bfloat16)
    for j in range(owners):
        out_ref, here = out_refs[j], slice(j * own, (j + 1) * own)
        out_ref[heads * width :, :] = stats[:, here]
        for h in range(heads):
            rows = slice(h * width, (h + 1) * width)
            keep, add = scales[h]
            mixed = acc_ref[h, :, start + j * own : start + (j + 1) * own] * keep[:, here]
            if add is not None:
                mixed = mixed + more_refs[j][rows, :].astype(jnp.float32) * add[:, here]
            out_ref[rows, :] = mixed.astype(jnp.bfloat16)


def pack(state, heads, own, start=0, more=()):
    acc, stat = state
    width, count = acc.shape[1], acc.shape[2]
    owners = (count - start) // own
    message = jax.ShapeDtypeStruct((heads * width + STAT_ROWS, own), jnp.bfloat16)
    return pl.pallas_call(
        functools.partial(pack_kernel, heads=heads, width=width, own=own, start=start, owners=owners),
        out_shape=(message,) * owners,
        in_specs=[VMEM] * (2 + len(more)),
        out_specs=(VMEM,) * owners,
        compiler_params=pltpu.CompilerParams(vmem_limit_bytes=4 * 2**20),
        name="pack",
    )(acc, stat, *more)


def merge_kernel(*refs, heads, width):
    in_refs, out_ref = refs[:-1], refs[-1]
    for h in range(heads):
        logs = [
            log_weight(part[heads * width :, :].astype(jnp.float32), h) for part in in_refs
        ]
        top = functools.reduce(jnp.maximum, logs)
        shares = [jnp.exp2(x - top) for x in logs]
        total = functools.reduce(jnp.add, shares)
        mixed = None
        for ref, share in zip(in_refs, shares):
            part = ref[h * width : (h + 1) * width, :].astype(jnp.float32) * (share / total)
            mixed = part if mixed is None else mixed + part
        out_ref[:, h * width : (h + 1) * width] = mixed.T.astype(jnp.bfloat16)


def merge(parts, heads, width):
    return pl.pallas_call(
        functools.partial(merge_kernel, heads=heads, width=width),
        out_shape=jax.ShapeDtypeStruct((parts[0].shape[1], heads * width), jnp.bfloat16),
        in_specs=[VMEM] * len(parts),
        out_specs=VMEM,
        compiler_params=pltpu.CompilerParams(vmem_limit_bytes=4 * 2**20),
        name="merge",
    )(*parts)


def body(queries, keys, values):
    own, heads, width = queries.shape
    n_x, n_z, n_col = (lax.axis_size(a) for a in ("x", "z", "col"))
    swap = functools.partial(lax.ppermute, axis_name="col", perm=[(c, n_col - 1 - c) for c in range(n_col)])
    along = [
        (z * n_col + c, (z + (1 if c == 0 else -1)) % n_z * n_col + c)
        for z in range(n_z)
        for c in range(n_col)
    ]
    forward = functools.partial(lax.ppermute, axis_name=("z", "col"), perm=along)
    here = jnp.concatenate([keys, values], axis=0).reshape(2 * own, heads * width)
    q = lax.optimization_barrier((queries, here))[0].reshape(own, heads * width)
    ahead = forward(here)
    other = swap(here)
    chunk = [ahead, forward(other)]

    q_mine = [q]
    for d in (1, n_x - 1, *range(2, n_x - 1)):
        q_mine.append(lax.ppermute(q, "x", [(x, (x + d) % n_x) for x in range(n_x)]))
    offsets = [0, 1, n_x - 1, *range(2, n_x - 1)]
    q_theirs = [swap(a) for a in q_mine]
    q_all = lay(q_mine + q_theirs, heads)

    state = fold(None, [here, *chunk], q_all)
    last = n_z // 2
    for _ in range(2, last):
        near = forward(chunk[0])
        chunk = [near, forward(chunk[1])]
        state = fold(state, chunk, q_all)
    share = q_all.shape[1] // n_col
    sent = [swap(a) for a in pack(state, heads, own, start=share)]
    chunk = forward(chunk[0])
    other = swap(chunk)
    mine = fold(state, [chunk], q_all, share)
    mine = fold(mine, [other], q_all, share)

    parts = pack(mine, heads, own, more=sent)
    home = [parts[0]]
    for d, part in zip(offsets[1:], parts[1:]):
        home.append(lax.ppermute(part, "x", [(x, (x - d) % n_x) for x in range(n_x)]))
    return merge(home, heads, width)


def solution(mesh):
    n_grp, n_row, n_col = mesh.devices.shape
    n_z = n_row // ROW_X
    split = Mesh(mesh.devices.reshape(n_grp, ROW_X, n_z, n_col), ("grp", "x", "z", "col"))
    everywhere = ("grp", "x", "z", "col")

    return jax.shard_map(
        body,
        mesh=split,
        in_specs=(P(everywhere, None, None),) * 3,
        out_specs=P(everywhere, None),
        check_vma=False,
    )
```
